512 devices in a mesh: cfg: 2 (over y_hi), win: 256 (over x, z, y_lo, core).
Axes of the slice: x: 4, y: 4 (y_hi: 2, y_lo: 2; y = y_hi * 2 + y_lo), z: 16, core: 2. Of those that a mesh axis runs over, the one named last changes fastest.
Arguments:
- latent: float32 [8192, 4, 32], P('win'), may hold values from -6 to 6
- text_kv: bfloat16 [2, 2, 120, 576], P(None, None, None, 'cfg'), may hold values from -200 to 200, as said below
- modulation: float32 [20, 4, 1152], replicated, may hold values from -3 to 3
- qkv_weight: bfloat16 [1152, 3, 576], P(None, None, 'cfg'), may hold values from -0.1875 to 0.1875
- out_weight: bfloat16 [576, 1152], P('cfg'), may hold values from -0.25 to 0.25
- patch_weight: bfloat16 [16, 1152], replicated, may hold values from -1.5 to 1.5
- final_weight: bfloat16 [1152, 16], replicated, may hold values from -0.1875 to 0.1875
- offsets: int32 [256], P('win'), may hold values from 1 to 16
- blend_weights: int32 [256], P('win'), may hold values from 1 to 4
- step_index: int32 [1], replicated, may hold values from 0 to 999
Outputs:
- previous: float32 [8192, 4, 32], P('win', None, 'cfg')
- noise: float32 [8192, 4, 32], P('win', None, 'cfg')
The draws below stay inside these ranges and needn't reach their ends.
Inputs may be any that keep to these rules, and one draw needn't show every extreme that they name: Window i starts offsets[i] columns before column i * 32. `text_kv`: keys and values of caption tokens.
All inputs are finite; a program needn't handle non-finite values.
Results may differ from the reference program's by a relative error of at most 0.024.
Values may be sent and summed in bfloat16 or wider, within the bound.
A program may use at most 64 MiB of HBM per device.

```python
import math
import jax
import jax.numpy as jnp
from jax import lax

D = 1152
HEAD_DIM = 72
CHANNELS = 4
CTX = 120
SLAB = 32
LAT_H = 32
STEPS = 20
ATTN = 576
LAT_W = 8192
N_WIN = 256


def draw_text_kv(key, part):
    base = jax.random.normal(jax.random.fold_in(key, 11), (2, 2, CTX, ATTN), jnp.float32)
    base = jnp.clip(base, -4.0, 4.0)
    return base.astype(jnp.bfloat16)


def set_ends(drawn, key, low, high):
    shape = drawn.shape
    index_at = [jax.random.randint(jax.random.fold_in(key, axis), (), 0, shape[axis]) for axis in range(len(shape))]
    drawn = drawn.at[tuple(index_at)].set(low)
    longest = shape.index(max(shape))
    index_at[longest] = (index_at[longest] + 1) % shape[longest]
    return drawn.at[tuple(index_at)].set(high)


def block_scale(key, shape, split, least, largest):
    level = 1.0
    for dim, parts in split:
        draws = jax.random.uniform(jax.random.fold_in(jax.random.fold_in(key, 6), dim), (parts,), jnp.float32, least / len(split), largest / len(split))
        level = level * jnp.repeat(jnp.exp(draws), shape[dim] // parts).reshape((-1,) + (1,) * (len(shape) - 1 - dim))
    return level


def normal_values(key, shape, scale, bound, shards=(), kind=jnp.bfloat16):
    entries = scale * jax.random.normal(key, shape, jnp.float32)
    if shards:
        entries = entries * block_scale(key, shape, shards, -0.22, 0.18)
    return jnp.clip(entries, -bound, bound).astype(kind)


def setup_inputs(seed: int = 0) -> dict:
    key_of = jax.random.split(jax.random.key(seed), 11)
    latent = normal_values(key_of[0], (LAT_W, CHANNELS, LAT_H), 1.0, 6.0, ((0, 256),), jnp.float32)
    text_kv = draw_text_kv(jax.random.fold_in(key_of[10], 71), 0)
    modulation = normal_values(key_of[2], (STEPS, 4, D), 0.5, 3.0, (), jnp.float32)
    qkv_weight = normal_values(key_of[3], (D, 3, ATTN), D ** -0.5, 0.1875, ((2, 2),))
    out_weight = normal_values(key_of[4], (ATTN, D), ATTN ** -0.5, 0.25, ((0, 2),))
    patch_weight = normal_values(key_of[5], (4 * CHANNELS, D), (4 * CHANNELS) ** -0.5, 1.5)
    final_weight = normal_values(key_of[6], (D, 4 * CHANNELS), D ** -0.5, 0.1875)
    offsets = set_ends(jax.random.randint(key_of[7], (N_WIN,), 1, SLAB // 2 + 1), jax.random.fold_in(key_of[7], 1), 1, (SLAB // 2 + 1) - 1).astype(jnp.int32)
    blend_weights = set_ends(jax.random.randint(key_of[8], (N_WIN,), 1, 5), jax.random.fold_in(key_of[8], 1), 1, 4).astype(jnp.int32)
    step_index = jax.random.randint(key_of[9], (1,), 0, 1000).astype(jnp.int32)
    return {"latent": latent, "text_kv": text_kv, "modulation": modulation, "qkv_weight": qkv_weight, "out_weight": out_weight, "patch_weight": patch_weight, "final_weight": final_weight, "offsets": offsets, "blend_weights": blend_weights, "step_index": step_index}


guidance_scale = 4.5
plan_length = 1000
norm_eps = 1e-06

def layer_norm(values):
    average = lax.optimization_barrier(jnp.mean(values, axis=-1, keepdims=True))
    centered = values - average
    variance = lax.optimization_barrier(jnp.mean(centered * centered, axis=-1, keepdims=True))
    return centered * lax.rsqrt(variance + norm_eps)

def positions(col_pairs, row_couples, model_width):
    quarter = model_width // 4
    frequency = jnp.exp(-math.log(10000.0) * jnp.arange(quarter, dtype=jnp.float32) / quarter)
    col_pos = jnp.arange(col_pairs, dtype=jnp.float32)[:, None] * frequency[None, :]
    row_pos = jnp.arange(row_couples, dtype=jnp.float32)[:, None] * frequency[None, :]
    col_part = jnp.concatenate([jnp.sin(col_pos), jnp.cos(col_pos)], axis=1)
    row_part = jnp.concatenate([jnp.sin(row_pos), jnp.cos(row_pos)], axis=1)
    half_width = model_width // 2
    pos_table = jnp.concatenate([jnp.broadcast_to(row_part[None, :, :], (col_pairs, row_couples, half_width)), jnp.broadcast_to(col_part[:, None, :], (col_pairs, row_couples, half_width))], axis=2)
    return pos_table.reshape(col_pairs * row_couples, model_width)

def plan(moment):
    train_grid = jnp.arange(plan_length, dtype=jnp.int32)
    beta_values = 0.0001 + (0.02 - 0.0001) * train_grid.astype(jnp.float32) / (plan_length - 1)
    alpha_bar = jnp.exp(jnp.cumsum(jnp.log(1.0 - beta_values)))
    stride = plan_length // STEPS
    earlier = moment - stride
    alpha_now = jnp.sum(jnp.where(train_grid == moment, alpha_bar, 0.0))
    alpha_before = jnp.sum(jnp.where(train_grid == earlier, alpha_bar, 0.0)) + jnp.where(earlier < 0, 1.0, 0.0)
    return (alpha_now, alpha_before)

def predict_pair(window, modulate, w_qkv, w_out, text_kv, patch_weight, final_weight):
    col_count, channels, row_count = window.shape
    col_pairs = col_count // 2
    row_couples = row_count // 2
    model_width = patch_weight.shape[1]
    attn_width = w_out.shape[0]
    half_attn = attn_width // 2
    head_count = attn_width // HEAD_DIM
    patches = window.reshape(col_pairs, 2, channels, row_couples, 2).transpose(0, 3, 1, 2, 4)
    patches = patches.reshape(col_pairs * row_couples, 4 * channels).astype(jnp.bfloat16)
    embedded = jnp.dot(patches, patch_weight, preferred_element_type=jnp.float32) + positions(col_pairs, row_couples, model_width)
    normed = (layer_norm(embedded) * (1.0 + modulate[1]) + modulate[0]).astype(jnp.bfloat16)
    projected = jnp.dot(normed, w_qkv, preferred_element_type=jnp.float32).astype(jnp.bfloat16)
    tokens = projected.shape[0]
    queries = projected[:, :attn_width].reshape(tokens, head_count, HEAD_DIM).astype(jnp.float32)
    results = []
    for branch_index in range(2):
        keys_all = jnp.concatenate([projected[:, attn_width:2 * attn_width], text_kv[branch_index, 0]], axis=0)
        keys_all = keys_all.reshape(-1, head_count, HEAD_DIM).astype(jnp.float32)
        values_all = jnp.concatenate([projected[:, 2 * attn_width:], text_kv[branch_index, 1]], axis=0)
        values_all = values_all.reshape(-1, head_count, HEAD_DIM).astype(jnp.float32)
        scores = jnp.einsum('qhd,khd->hqk', queries, keys_all) * (1.0 / math.sqrt(HEAD_DIM))
        highest = lax.optimization_barrier(jnp.max(scores, axis=-1, keepdims=True))
        exponent = jnp.exp(scores - highest)
        soft_weights = (exponent / lax.optimization_barrier(jnp.sum(exponent, axis=-1, keepdims=True))).astype(jnp.bfloat16)
        attended = jnp.einsum('hqk,khd->qhd', soft_weights.astype(jnp.float32), values_all)
        attended = attended.reshape(tokens, attn_width).astype(jnp.bfloat16)
        part_low = jnp.dot(attended[:, :half_attn], w_out[:half_attn], preferred_element_type=jnp.float32).astype(jnp.bfloat16)
        part_high = jnp.dot(attended[:, half_attn:], w_out[half_attn:], preferred_element_type=jnp.float32).astype(jnp.bfloat16)
        part_low, part_high = lax.optimization_barrier((part_low, part_high))
        mixed_sum = part_low.astype(jnp.float32) + part_high.astype(jnp.float32)
        residual = embedded + modulate[2] * mixed_sum
        final_norm = (layer_norm(residual) * (1.0 + modulate[3])).astype(jnp.bfloat16)
        noise_tokens = jnp.dot(final_norm, final_weight, preferred_element_type=jnp.float32)
        unpacked = noise_tokens.reshape(col_pairs, row_couples, 2, channels, 2).transpose(0, 2, 3, 1, 4)
        results.append(unpacked.reshape(col_count, channels, row_count))
    return (results[0], results[1])

def reference(latent, text_kv, modulation, qkv_weight, out_weight, patch_weight, final_weight, offsets, blend_weights, step_index):
    model_width = patch_weight.shape[1]
    attn_width = out_weight.shape[0]
    w_qkv = qkv_weight.reshape(model_width, 3 * attn_width)
    moment = step_index[0]
    selected = jnp.arange(STEPS, dtype=jnp.int32) == moment * STEPS // plan_length
    modulate = lax.optimization_barrier(jnp.sum(jnp.where(selected[:, None, None], modulation, 0.0), axis=0))
    columns_all = latent.shape[0]
    span_index = jnp.arange(2 * SLAB, dtype=jnp.int32)

    def one_window(window_index):
        start_at = window_index * SLAB - offsets[window_index]
        column_list = ((start_at + span_index) % columns_all).astype(jnp.int32)
        window = jnp.take(latent, column_list, axis=0)
        conditional, unconditional = predict_pair(window, modulate, w_qkv, out_weight, text_kv, patch_weight, final_weight)
        return unconditional + guidance_scale * (conditional - unconditional)
    guided = lax.map(one_window, jnp.arange(N_WIN, dtype=jnp.int32))
    weight_values = blend_weights.astype(jnp.float32)
    window_columns = (jnp.arange(N_WIN, dtype=jnp.int32)[:, None] * SLAB - offsets[:, None] + span_index[None, :]) % columns_all
    window_columns = window_columns.reshape(-1).astype(jnp.int32)
    weighted = (weight_values[:, None, None, None] * guided).reshape(-1, CHANNELS, LAT_H)
    numerator = jnp.zeros_like(latent).at[window_columns].add(weighted)
    spread_weights = jnp.broadcast_to(weight_values[:, None], (N_WIN, 2 * SLAB)).reshape(-1)
    denominator = jnp.zeros((columns_all,), latent.dtype).at[window_columns].add(spread_weights)
    blended = numerator / denominator[:, None, None]
    alpha_now, alpha_before = plan(moment)
    previous = jnp.sqrt(alpha_before) * (latent - jnp.sqrt(1.0 - alpha_now) * blended) / jnp.sqrt(alpha_now) + jnp.sqrt(1.0 - alpha_before) * blended
    return (previous, blended)
```

```python
import functools
import math

import jax
import jax.numpy as jnp
import numpy as np
from jax import lax
from jax.experimental import pallas as pl
from jax.experimental.pallas import tpu as pltpu
from jax.sharding import PartitionSpec as P

HEAD_DIM = 72
STEPS = 20

guidance_scale = 4.5
plan_length = 1000
norm_eps = 1e-06

MESH = pl.DeviceIdType.MESH
F32 = jnp.float32
BF16 = jnp.bfloat16


def position_tables(col_pairs, row_couples, model_width):
    quarter = model_width // 4
    frequency = np.exp(-math.log(10000.0) * np.arange(quarter) / quarter)

    def part(count):
        angle = np.arange(count)[:, None] * frequency[None, :]
        return np.concatenate([np.sin(angle), np.cos(angle)], axis=1)

    row_pos = np.zeros((row_couples, model_width), np.float32)
    row_pos[:, : model_width // 2] = part(row_couples)
    col_pos = np.zeros((col_pairs, model_width), np.float32)
    col_pos[:, model_width // 2 :] = part(col_pairs)
    return row_pos, col_pos


def plan_tables():
    beta = 1e-4 + (0.02 - 1e-4) * np.arange(plan_length) / (plan_length - 1)
    now = np.exp(np.cumsum(np.log(1.0 - beta)))
    stride = plan_length // STEPS
    before = np.concatenate([np.ones(stride), now[:-stride]])
    keep = np.sqrt(before) / np.sqrt(now)
    step = np.sqrt(1.0 - before) - keep * np.sqrt(1.0 - now)
    return keep.astype(np.float32), step.astype(np.float32)


def nt(a, b):
    return lax.dot_general(a, b, (((1,), (1,)), ((), ())), preferred_element_type=F32)


def tn(a, b):
    return lax.dot_general(a, b, (((0,), (0,)), ((), ())), preferred_element_type=F32)


def nn(a, b):
    return jnp.dot(a, b, preferred_element_type=F32)


def exact(a, b):
    return jnp.dot(a, b, preferred_element_type=F32, precision=lax.Precision.HIGHEST)


def iota(shape, dim):
    return lax.broadcasted_iota(jnp.int32, shape, dim)


def kernel(
    n_win,
    off_ref,
    blend_ref,
    step_ref,
    keep_ref,
    stepc_ref,
    lat_hbm,
    text_hbm,
    mod_hbm,
    qkv_hbm,
    wout_hbm,
    pw_hbm,
    fw_hbm,
    rowpos_hbm,
    colpos_hbm,
    prev_ref,
    noise_ref,
    lat,
    text,
    mod,
    wqkv,
    wown,
    woth,
    pw,
    fw,
    rowpos,
    colpos,
    slabs,
    win32,
    emb,
    normed,
    proj,
    kall,
    vall,
    att_send,
    att_recv,
    att_own,
    mixed,
    blend_own,
    blend_send,
    blend_recv,
    local_sem,
    send_sem,
    recv_sem,
):
    c = lax.axis_index("cfg")
    w = lax.axis_index("win")
    right = lax.rem(w + 1, n_win)
    left = lax.rem(w + n_win - 1, n_win)
    first = c == 0

    names = (
        (lat_hbm, lat),
        (pw_hbm, pw),
        (rowpos_hbm, rowpos),
        (colpos_hbm, colpos),
        (mod_hbm, mod),
        (qkv_hbm, wqkv),
        (text_hbm, text),
        (wout_hbm, wown),
        (fw_hbm, fw),
    )
    loads = [
        pltpu.make_async_copy(src, dst, local_sem.at[i]) for i, (src, dst) in enumerate(names)
    ]
    barrier = pltpu.get_barrier_semaphore()
    for target in ((c, left), (c, right), (1 - c, w)):
        pl.semaphore_signal(barrier, inc=1, device_id=target, device_id_type=MESH)
    for load in loads:
        load.start()
    lat_load, pw_load, row_load, col_load, mod_load, qkv_load, text_load, own_load, fw_load = loads

    lat_load.wait()
    slab = jnp.transpose(lat[...])
    slabs[1] = slab.astype(BF16)

    pl.semaphore_wait(barrier, 3)

    def send(i, src, dst, target):
        copy = pltpu.make_async_remote_copy(
            src_ref=src,
            dst_ref=dst,
            send_sem=send_sem.at[i],
            recv_sem=recv_sem.at[i],
            device_id=target,
            device_id_type=MESH,
        )
        copy.start()
        return copy

    to_right = send(0, slabs.at[1], slabs.at[0], (c, right))
    to_left = send(1, slabs.at[1], slabs.at[2], (c, left))
    weights = send(2, wout_hbm, woth, (1 - c, w))

    half_rows = slab.shape[0] // 2
    own_rows = jnp.where(first, slab[:half_rows], slab[half_rows:])
    lane = iota((half_rows, 128), 1)
    picked = jnp.concatenate(
        [jnp.where(lane % 4 == ch, own_rows, 0.0) for ch in range(4)], axis=0
    )
    column_of = (iota((128, 128), 0) // 4 == iota((128, 128), 1)).astype(F32)
    lat_out = exact(picked, column_of)

    off = off_ref[0]
    moment = step_ref[0]

    src = iota((384, 256), 0)
    dst = iota((384, 256), 1)
    shift = (src == dst + 4 * (32 - off)).astype(F32).astype(BF16)

    pw_load.wait()
    feature = iota((256, 16), 0)
    wanted = (feature % 8) // 4 * 8 + feature % 4 * 2 + feature // 128
    embed_w = nn((iota((256, 16), 1) == wanted).astype(F32).astype(BF16), pw[...]).astype(BF16)

    row_load.wait()
    col_load.wait()
    mod_load.wait()
    modulate = mod[lax.div(moment * STEPS, plan_length)]
    mod_shift = modulate[0:1]
    mod_scale = 1.0 + modulate[1:2]
    gate = modulate[2:3]
    out_scale = 1.0 + modulate[3:4]

    text_load.wait()
    heads = 4
    for b in range(2):
        keys = text[b, 0].astype(F32)
        vals = text[b, 1].astype(F32)
        zeros_k = jnp.zeros((8, HEAD_DIM), F32)
        for h in range(heads):
            part = keys[h * HEAD_DIM : (h + 1) * HEAD_DIM]
            kt = jnp.transpose(part)
            kall[h, 512 + 128 * b : 640 + 128 * b, :] = jnp.concatenate(
                [kt, zeros_k], axis=0
            ).astype(BF16)
            vt = jnp.concatenate(
                [vals[h * HEAD_DIM : (h + 1) * HEAD_DIM], jnp.ones((8, 120), F32)], axis=0
            )
            vall[h, :, 512 + 128 * b : 632 + 128 * b] = vt.astype(BF16)
            vall[h, :, 632 + 128 * b : 640 + 128 * b] = jnp.zeros((80, 8), BF16)

    to_right.wait_recv()
    to_left.wait_recv()
    all_slabs = jnp.concatenate([slabs[0], slabs[1], slabs[2]], axis=1)
    window = nn(all_slabs, shift)
    win32[0] = window[:, :128]
    win32[1] = window[:, 128:]

    token_mask = iota((128, 128), 0) // 8 == iota((128, 128), 1) // 8
    for half in range(2):
        groups = []
        for g in range(2):
            both = []
            for dh in range(2):
                low = win32[g, pl.ds(dh, 8, stride=2), :]
                high = win32[g, pl.ds(16 + dh, 8, stride=2), :]
                piece = jnp.where(first, high, low) if half == 0 else jnp.where(first, low, high)
                both.append(
                    jnp.where(token_mask, jnp.concatenate([piece] * 16, axis=0), 0.0)
                )
            groups.append(jnp.concatenate(both, axis=1))
        lhs = jnp.concatenate(groups, axis=0).astype(BF16)
        emb[half * 256 : (half + 1) * 256, :] = nn(lhs, embed_w)

    rp = rowpos[...]
    rp_half = (jnp.where(first, rp[8:], rp[:8]), jnp.where(first, rp[:8], rp[8:]))
    model_width = emb.shape[1]

    def center(values):
        centered = values - jnp.mean(values, axis=-1, keepdims=True)
        variance = jnp.mean(centered * centered, axis=-1, keepdims=True)
        return centered * lax.rsqrt(variance + norm_eps)

    for half in range(2):
        for chunk in range(8):
            at = half * 256 + chunk * 32
            values = emb[at : at + 32, :].reshape(4, 8, model_width)
            values = values + rp_half[half][None]
            values = values + colpos[chunk * 4 : chunk * 4 + 4, :].reshape(4, 1, model_width)
            values = values.reshape(32, model_width)
            if half == 1:
                emb[at : at + 32, :] = values
            normed[at : at + 32, :] = (center(values) * mod_scale + mod_shift).astype(BF16)

    qkv_load.wait()
    proj[...] = nt(wqkv[...], normed[...])

    for h in range(heads):
        kt = proj[288 + h * HEAD_DIM : 288 + (h + 1) * HEAD_DIM, :]
        kall[h, 0:512, :] = jnp.transpose(kt).astype(BF16)
        vt = proj[576 + h * HEAD_DIM : 576 + (h + 1) * HEAD_DIM, :]
        vall[h, :, 0:512] = jnp.concatenate([vt, jnp.ones((8, 512), F32)], axis=0).astype(BF16)

    factor = math.log2(math.e) / math.sqrt(HEAD_DIM)

    def attend(h, half):
        q = (
            proj[h * HEAD_DIM : (h + 1) * HEAD_DIM, half * 256 : (half + 1) * 256] * factor
        ).astype(BF16)
        scores = nn(kall[h], q)
        own = scores[:512]
        own_max = jnp.max(own, axis=0, keepdims=True)
        own_exp = jnp.exp2(own - own_max).astype(BF16)
        own_out = nn(vall[h, :, 0:512], own_exp)
        result = []
        for b in range(2):
            cap = scores[512 + 128 * b : 632 + 128 * b]
            cap_max = jnp.max(cap, axis=0, keepdims=True)
            cap_exp = jnp.concatenate(
                [jnp.exp2(cap - cap_max), jnp.zeros((8, 256), F32)], axis=0
            ).astype(BF16)
            cap_out = nn(vall[h, :, 512 + 128 * b : 640 + 128 * b], cap_exp)
            top = jnp.maximum(own_max, cap_max)
            w_own = jnp.exp2(own_max - top)
            w_cap = jnp.exp2(cap_max - top)
            total = w_own * own_out[72:73] + w_cap * cap_out[72:73]
            w_own = w_own / total
            w_cap = w_cap / total
            result.append(own_out[:72] * w_own + cap_out[:72] * w_cap)
        return result

    att_copies = []
    for half in range(2):
        for pair in range(2):
            one = attend(2 * pair, half)
            two = attend(2 * pair + 1, half)
            for b in range(2):
                both = jnp.concatenate([one[b], two[b]], axis=0).astype(BF16)
                if half == 0:
                    att_send[pair, :, b * 256 : (b + 1) * 256] = both
                else:
                    att_own[pair * 144 : (pair + 1) * 144, b * 256 : (b + 1) * 256] = both
            if half == 0:
                att_copies.append(
                    send(3 + pair, att_send.at[pair], att_recv.at[pair], (1 - c, w))
                )

    own_load.wait()
    mixed[...] = tn(att_own[...], wown[...])
    weights.wait_recv()
    for copy in att_copies:
        copy.wait_recv()
    other = jnp.concatenate([att_recv[0], att_recv[1]], axis=0)
    mixed[...] += tn(other, woth[...])

    fw_load.wait()
    eps = []
    for b in range(2):
        for chunk in range(8):
            at = chunk * 32
            values = emb[256 + at : 288 + at, :] + gate * mixed[b * 256 + at : b * 256 + at + 32, :]
            normed[b * 256 + at : b * 256 + at + 32, :] = (center(values) * out_scale).astype(BF16)
    for b in range(2):
        eps.append(nt(normed[b * 256 : (b + 1) * 256, :], fw[...]))
    blend = blend_ref[0].astype(F32)
    guided = (eps[1] + guidance_scale * (eps[0] - eps[1])) * blend
    guided_t = jnp.transpose(guided)

    start = 16 - off
    row = iota((16, 256), 0)
    keep = (iota((16, 256), 1) % 8) == (row // 2)
    spread = None
    for dw in range(2):
        blocks = []
        for ch in range(4):
            f = dw * 8 + ch * 2
            even = jnp.broadcast_to(guided_t[f : f + 1], (16, 256))
            odd = jnp.broadcast_to(guided_t[f + 1 : f + 2], (16, 256))
            blocks.append(jnp.where(keep, jnp.where(row % 2 == 0, even, odd), 0.0))
        place = (iota((256, 128), 1) == (iota((256, 128), 0) // 8) * 2 + dw + start).astype(F32)
        term = exact(jnp.concatenate(blocks, axis=0), place)
        spread = term if spread is None else spread + term
    lanes = iota((8, 128), 1)
    cover = jnp.where((lanes >= start) & (lanes < start + 64), blend, 0.0)
    laid = jnp.concatenate([spread, cover], axis=0)
    blend_send[0] = pltpu.roll(laid, 128 - 48, axis=1)
    blend_send[1] = pltpu.roll(laid, 16, axis=1)
    blend_right = send(5, blend_send.at[0], blend_recv.at[0], (c, right))
    blend_left = send(6, blend_send.at[1], blend_recv.at[1], (c, left))
    kept = pltpu.roll(laid, 128 - 16, axis=1)
    blend_right.wait_recv()
    blend_left.wait_recv()
    from_left = blend_recv[0]
    from_right = blend_recv[1]
    lanes72 = iota((72, 128), 1)
    total = (
        kept
        + jnp.where(lanes72 < 32, from_left, 0.0)
        + jnp.where((lanes72 >= 16) & (lanes72 < 32), from_right, 0.0)
    )
    noise = total[:64] / total[64:65]
    noise_ref[...] = noise[:, :32]
    prev_ref[...] = (keep_ref[moment] * lat_out + stepc_ref[moment] * noise)[:, :32]

    for copy in [to_right, to_left, weights, blend_right, blend_left] + att_copies:
        copy.wait_send()


def on_device(
    n_win,
    latent,
    text_kv,
    modulation,
    qkv_weight,
    out_weight,
    patch_weight,
    final_weight,
    offsets,
    blend_weights,
    step_index,
):
    slab_cols, channels, row_count = latent.shape
    model_width = patch_weight.shape[1]
    half_attn = out_weight.shape[0]
    row_pos, col_pos = position_tables(slab_cols, row_count // 2, model_width)
    keep, step = plan_tables()
    lat = latent.reshape(slab_cols * channels, row_count)
    text = text_kv.transpose(0, 1, 3, 2)
    qkv = qkv_weight.transpose(1, 2, 0).reshape(3 * half_attn, model_width)
    fw = final_weight.T
    hbm = pl.BlockSpec(memory_space=pltpu.HBM)
    smem = pl.BlockSpec(memory_space=pltpu.SMEM)
    vmem = pl.BlockSpec(memory_space=pltpu.VMEM)
    half_rows = row_count // 2
    out = jax.ShapeDtypeStruct((channels * half_rows, slab_cols), F32)
    prev, noise = pl.pallas_call(
        functools.partial(kernel, n_win),
        out_shape=(out, out),
        in_specs=[smem] * 5 + [hbm] * 9,
        out_specs=(vmem, vmem),
        scratch_shapes=[
            pltpu.VMEM(lat.shape, F32),
            pltpu.VMEM(text.shape, BF16),
            pltpu.VMEM(modulation.shape, F32),
            pltpu.VMEM(qkv.shape, BF16),
            pltpu.VMEM(out_weight.shape, BF16),
            pltpu.VMEM(out_weight.shape, BF16),
            pltpu.VMEM(patch_weight.shape, BF16),
            pltpu.VMEM(fw.shape, BF16),
            pltpu.VMEM(row_pos.shape, F32),
            pltpu.VMEM(col_pos.shape, F32),
            pltpu.VMEM((3, 32, 128), BF16),
            pltpu.VMEM((2, 32, 128), F32),
            pltpu.VMEM((512, model_width), F32),
            pltpu.VMEM((512, model_width), BF16),
            pltpu.VMEM((3 * half_attn, 512), F32),
            pltpu.VMEM((4, 768, HEAD_DIM), BF16),
            pltpu.VMEM((4, 80, 768), BF16),
            pltpu.VMEM((2, 144, 512), BF16),
            pltpu.VMEM((2, 144, 512), BF16),
            pltpu.VMEM((288, 512), BF16),
            pltpu.VMEM((512, model_width), F32),
            pltpu.VMEM((72, 128), F32),
            pltpu.VMEM((2, 72, 128), F32),
            pltpu.VMEM((2, 72, 128), F32),
            pltpu.SemaphoreType.DMA((9,)),
            pltpu.SemaphoreType.DMA((7,)),
            pltpu.SemaphoreType.DMA((7,)),
        ],
        compiler_params=pltpu.CompilerParams(
            collective_id=0, has_side_effects=True, vmem_limit_bytes=56 * 1024 * 1024
        ),
    )(
        offsets,
        blend_weights,
        step_index,
        jnp.asarray(keep),
        jnp.asarray(step),
        lat,
        text,
        modulation,
        qkv,
        out_weight,
        patch_weight,
        fw,
        jnp.asarray(row_pos),
        jnp.asarray(col_pos),
    )

    def placed(array):
        return array.reshape(channels, half_rows, slab_cols).transpose(2, 0, 1)

    return placed(prev), placed(noise)


def solution(mesh):
    in_specs = (
        P("win", None, None),
        P(None, None, None, "cfg"),
        P(),
        P(None, None, "cfg"),
        P("cfg", None),
        P(),
        P(),
        P("win"),
        P("win"),
        P(),
    )
    out_specs = (P("win", None, "cfg"), P("win", None, "cfg"))
    return jax.shard_map(
        functools.partial(on_device, mesh.shape["win"]),
        mesh=mesh,
        in_specs=in_specs,
        out_specs=out_specs,
        check_vma=False,
    )
```
